32 devices in a mesh: section: 2 (over y), ep: 16 (over z, x, core).
Axes of the slice: x: 2, y: 2, z: 4, core: 2. Of those that a mesh axis runs over, the one named last changes fastest.
Arguments:
- inputs: bfloat16 [2, 2048, 1536], P('section', 'ep'), may hold values from -6 to 6
- upstream: bfloat16 [2, 2048, 1536], P('section', 'ep'), may hold values from -6 to 6
- gate_saved: bfloat16 [2, 2048, 8, 384], P('section', 'ep'), may hold values from -6 to 6
- expert_ids: int32 [2, 2048, 8], P('section', 'ep'), may hold values from 0 to 31, all different within a row; in each aligned block of 128 rows (0 to 127, 128 to 255, ..., all dimensions but the last counted through in order) at most 48 rows name the same one
- route_weights: float32 [2, 2048, 8], P('section', 'ep'), may hold values from 0.05 to 0.5
- w_up: bfloat16 [2, 32, 1536, 384], P('section', 'ep'), may hold values from -0.15625 to 0.15625
- w_down: bfloat16 [2, 32, 384, 1536], P('section', 'ep'), may hold values from -0.3125 to 0.3125
Outputs:
- delivered: bfloat16 [2, 2048, 1536], P('section', 'ep')
- grad_up: bfloat16 [2, 32, 1536, 384], P('section', 'ep')
- grad_down: bfloat16 [2, 32, 384, 1536], P('section', 'ep')
The draws below stay inside these ranges and needn't reach their ends.
Inputs may be any that keep to these rules, and one draw needn't show every extreme that they name: `expert_ids`: each row names 8 different experts. In the rows of one device no expert is named more than 48 times, and in every draw some expert is named exactly 48 times in the rows of some device; every expert is named somewhere.
All inputs are finite; a program needn't handle non-finite values.
Results may differ from the reference program's by a relative error of at most 0.012.
Values may be sent and summed in bfloat16 or wider, within the bound.
No kernel may reach another device: no remote copies, remote signals or barrier semaphores. Data moves between devices by JAX's collectives and lax.ppermute only.
A program may use at most 192 MiB of HBM per device.

```python
import math
import jax
import jax.numpy as jnp
import numpy as np
from jax import lax

D = 1536
FF = 384
TOP = 8
TOK_DEV = 128
EXPERTS = 32
TOKENS = 2048
CAP = 48
N_SECTION = 2
N_EP = 16


def level_of(stream_key, shape, split, least, high):
    loudness, own = 1.0, jax.random.fold_in(stream_key, 6)
    for dim, parts in split:
        heights = jnp.exp(jax.random.uniform(jax.random.fold_in(own, dim), (parts,), jnp.float32, least / len(split), high / len(split)))
        loudness = loudness * jnp.repeat(heights, shape[dim] // parts).reshape([-1 if axis == dim else 1 for axis in range(len(shape))])
    return loudness


def assign_block(key, own, number, rows, amount, top, most, skew):
    order = jax.random.permutation(key, amount)
    packed, common = load_shares(amount, rows * top, most, skew, True), load_shares(amount, rows * top, most, skew, False)
    places = jnp.arange(amount)

    def named(sizes, rotation):
        used = int((sizes > 0).sum())
        fixed = max(1, used // 4)
        shifted = fixed + (places - fixed + rotation * (used - fixed)) % max(1, amount - fixed)
        return jnp.zeros((amount,), jnp.int32).at[order[jnp.where(places < fixed, places, shifted)]].set(jnp.asarray(sizes, jnp.int32))

    sizes = jnp.where(number % 4 == 0, named(packed, number // 4), named(common, number - number // 4 - 1))
    mixed = jax.random.permutation(jax.random.fold_in(own, 3), amount)
    donor, taker = mixed[0:amount // 2 * 2:2], mixed[1:amount // 2 * 2:2]
    slack = jnp.minimum(sizes[donor] - 1, most - sizes[taker]) // 2
    slack = jnp.where((donor == order[0]) | (taker == order[0]) | (sizes[taker] == 0), 0, jnp.maximum(slack, 0))
    shifted = jax.random.randint(jax.random.fold_in(own, 4), (amount // 2,), 0, 1 << 20) % (slack + 1)
    sizes = sizes.at[donor].add(-shifted).at[taker].add(shifted)
    labels = jnp.searchsorted(jnp.cumsum(sizes), jnp.arange(rows * top), side="right").astype(jnp.int32)
    table = labels.reshape(top, rows).T
    table = table[jax.random.permutation(jax.random.fold_in(own, 1), rows)]
    rotation = jax.random.randint(jax.random.fold_in(own, 2), (rows, 1), 0, top)
    return jnp.take_along_axis(table, (jnp.arange(top)[None, :] + rotation) % top, axis=1)


def load_shares(amount, total, most, slope, full):
    portions = [(1 << 20) // math.isqrt(rank ** slope) + 1 for rank in range(1, amount + 1)]
    largest = most if full else min(most, max(-(-total // amount), total * portions[0] // sum(portions)))
    least = 1 if total - largest >= amount - 1 else 0
    holding, surplus = [largest] + [least] * (amount - 1), total - largest - least * (amount - 1)
    while surplus > 0:
        free = [i for i in range(1, amount) if holding[i] < largest] or [i for i in range(1, amount) if holding[i] < most]
        whole, left = sum([portions[i] for i in free]), surplus
        for i in free:
            extra = min(most - holding[i], max(1, left * portions[i] // whole), surplus)
            holding[i] = holding[i] + extra
            surplus = surplus - extra
    return np.array(holding)


def gaussian(key, dims, deviation, limit, cuts=(), kind=jnp.bfloat16):
    result = jax.random.normal(key, dims, jnp.float32) * deviation
    if len(cuts) > 0:
        result = level_of(key, dims, cuts, -0.22, 0.18) * result
    return jnp.clip(result, min=-limit, max=limit).astype(kind)


def setup_inputs(seed: int = 0) -> dict:
    arg_keys = jax.random.split(jax.random.key(seed), 8)
    inputs = gaussian(arg_keys[0], (N_SECTION, TOKENS, D), 1.0, 6.0, ((0, 2), (1, 16)))
    upstream = gaussian(arg_keys[1], (N_SECTION, TOKENS, D), 1.0, 6.0, ((0, 2), (1, 16)))
    gate_saved = gaussian(arg_keys[2], (N_SECTION, TOKENS, TOP, FF), 1.5, 6.0, ((0, 2), (1, 16)))
    expert_ids_keys = jax.random.split(jax.random.fold_in(arg_keys[3], 1), N_SECTION * TOKENS // TOK_DEV)
    expert_ids_turns = jax.random.permutation(jax.random.fold_in(arg_keys[3], 3), N_SECTION * TOKENS // TOK_DEV)
    expert_ids = jax.vmap(lambda own, number: assign_block(jax.random.fold_in(arg_keys[3], 2), own, number, TOK_DEV, EXPERTS, TOP, CAP, 2))(expert_ids_keys, expert_ids_turns).reshape((N_SECTION, TOKENS, TOP))
    route_weights = jnp.clip(jnp.exp(math.log(0.5) - 2.3025851 * jax.random.uniform(arg_keys[4], (N_SECTION, TOKENS, TOP), jnp.float32) ** level_of(arg_keys[4], (N_SECTION, TOKENS, TOP), ((0, 2), (1, 16)), -0.2, 0.2)), 0.05, 0.5)
    w_up = gaussian(arg_keys[5], (N_SECTION, EXPERTS, D, FF), D ** -0.5, 0.15625, ((0, 2), (1, 16)))
    w_down = gaussian(arg_keys[6], (N_SECTION, EXPERTS, FF, D), FF ** -0.5, 0.3125, ((0, 2), (1, 16)))
    return {"inputs": inputs, "upstream": upstream, "gate_saved": gate_saved, "expert_ids": expert_ids, "route_weights": route_weights, "w_up": w_up, "w_down": w_down}


def one_section(operands):
    tokens_here, cotangent, gate_layer, id_layer, weight_layer, up_layer, down_layer = operands
    rows_block = TOK_DEV * TOP
    flat_ids = id_layer.reshape(N_EP, rows_block)
    onehot = (flat_ids[:, :, None] == jnp.arange(EXPERTS, dtype=jnp.int32)[None, None, :]).astype(jnp.int32)
    position = jnp.sum(jnp.cumsum(onehot, axis=1) * onehot, axis=2) - 1
    sources = jnp.arange(N_EP, dtype=jnp.int32)[:, None]
    slot_index = (sources * CAP + position).astype(jnp.int32)
    flat_index = jnp.arange(N_EP * rows_block, dtype=jnp.int32).reshape(N_EP, rows_block)
    table = jnp.full((EXPERTS, N_EP * CAP), N_EP * rows_block, jnp.int32)
    table = table.at[flat_ids, slot_index].set(flat_index)
    gate_flat = gate_layer.reshape(TOKENS * TOP, FF)
    weight_flat = weight_layer.reshape(TOKENS * TOP)

    def per_expert(carry, expert_args):
        slot_rows, up_weight, down_weight = expert_args
        token_of = (slot_rows // TOP).astype(jnp.int32)
        x_rows = jnp.take(tokens_here, token_of, axis=0, mode="fill", fill_value=0)
        gate_rows = jnp.take(gate_flat, slot_rows, axis=0, mode="fill", fill_value=0)
        scale_rows = jnp.take(weight_flat, slot_rows, axis=0, mode="fill", fill_value=0)
        cot_rows = jnp.take(cotangent, token_of, axis=0, mode="fill", fill_value=0)
        scaled = (scale_rows[:, None] * cot_rows.astype(jnp.float32)).astype(jnp.bfloat16)
        activation = jax.nn.silu(gate_rows.astype(jnp.float32))
        up_value = jnp.dot(x_rows, up_weight, preferred_element_type=jnp.float32)
        hidden = (activation * up_value).astype(jnp.bfloat16)
        grad_down = jnp.dot(hidden.T, scaled, preferred_element_type=jnp.float32)
        grad_hidden = jnp.dot(scaled, down_weight.T, preferred_element_type=jnp.float32)
        grad_rows = (grad_hidden * activation).astype(jnp.bfloat16)
        grad_up = jnp.dot(x_rows.T, grad_rows, preferred_element_type=jnp.float32)
        slot_grad = jnp.dot(grad_rows, up_weight.T, preferred_element_type=jnp.float32).astype(jnp.bfloat16)
        carry = carry.at[token_of].add(slot_grad.astype(jnp.float32), mode="drop")
        return carry, (grad_up.astype(jnp.bfloat16), grad_down.astype(jnp.bfloat16))

    start = jnp.zeros((TOKENS, D), jnp.float32)
    layer_grad, grads = lax.scan(per_expert, start, (table, up_layer, down_layer))
    return layer_grad.astype(jnp.bfloat16), grads[0], grads[1]


def reference(inputs, upstream, gate_saved, expert_ids, route_weights, w_up, w_down):
    cot_all = jnp.roll(upstream, -1, axis=0)
    layer_grads, grad_up, grad_down = lax.map(one_section, (inputs, cot_all, gate_saved, expert_ids, route_weights, w_up, w_down))
    delivered = jnp.roll(layer_grads, -1, axis=0)
    return delivered, grad_up, grad_down
```

```python
import functools

import jax
import jax.numpy as jnp
from jax import lax
from jax.experimental import pallas as pl
from jax.experimental.pallas import tpu as pltpu
from jax.sharding import PartitionSpec as P


F32 = jnp.float32
BF16 = jnp.bfloat16
EXTRA = 8
NT = (((1,), (1,)), ((), ()))
TN = (((0,), (0,)), ((), ()))


def dot(a, b, dims=(((1,), (0,)), ((), ()))):
    return lax.dot_general(a, b, dims, preferred_element_type=F32)


class Grid:
    def __init__(self):
        self.sections = lax.axis_size("section")
        self.size = lax.axis_size("ep")
        self.chips = self.size // 2
        bits = self.chips.bit_length() - 1
        self.z = 1 << ((bits + 1) // 2)
        self.x = self.chips // self.z

    def move(self, block, target, shift=0):
        pairs = []
        for s in range(self.sections):
            for i in range(self.size):
                to = target(i // 2 // self.x, i // 2 % self.x, i % 2)
                if to is not None:
                    z, x, core = to
                    there = (z * self.x + x) * 2 + core
                    pairs.append((s * self.size + i, (s + shift) % self.sections * self.size + there))
        return lax.ppermute(block, ("section", "ep"), pairs)


def after(value, *others):
    return lax.optimization_barrier((value, *others))[0]


def prep_kernel(top, cap, local, ids_ref, act_ref, *out_refs):
    index = lax.axis_index("ep")
    chip, core = index // 2, index % 2
    rows = act_ref.shape[0]
    experts = len(out_refs) * 2 * local
    ids = ids_ref[...]
    named = lax.broadcasted_iota(jnp.int32, (experts, rows), 0) == ids
    upper = lax.broadcasted_iota(jnp.int32, (rows, rows), 0) <= lax.broadcasted_iota(jnp.int32, (rows, rows), 1)
    count = dot(named.astype(F32).astype(BF16), upper.astype(F32).astype(BF16))
    position = jnp.sum(jnp.where(named, count, 0.0), axis=0, keepdims=True).astype(jnp.int32) - 1
    slot = ids * cap + position
    half = local * cap
    place = lax.broadcasted_iota(jnp.int32, (2 * half, 1), 0)
    token = (lax.broadcasted_iota(jnp.int32, (EXTRA, rows), 1) // top + 1).astype(F32).astype(BF16)
    for k, out_ref in enumerate(out_refs):
        first = ((chip ^ k) * 2 + core) * half
        second = ((chip ^ k) * 2 + 1 - core) * half
        mine = jnp.where(place < half, place + first, place - half + second)
        onehot = (mine == slot).astype(F32).astype(BF16)
        out_ref[0:2 * half, :] = dot(onehot, act_ref[...]).astype(BF16)
        out_ref[2 * half:2 * half + EXTRA, :] = jnp.zeros((EXTRA, out_ref.shape[1]), BF16)
        out_ref[2 * half:2 * half + EXTRA, 0:2 * half] = dot(token, onehot, NT).astype(BF16)


def prep(ids_row, act, top, cap, local, chips):
    rows, width = act.shape
    shape = jax.ShapeDtypeStruct((2 * local * cap + EXTRA, width), BF16)
    return pl.pallas_call(
        functools.partial(prep_kernel, top, cap, local),
        out_shape=[shape] * chips,
        name="prep",
        compiler_params=pltpu.CompilerParams(vmem_limit_bytes=24 << 20),
        cost_estimate=pl.CostEstimate(
            flops=4 * rows * rows * width, bytes_accessed=4 * rows * width, transcendentals=0
        ),
    )(ids_row, act)


def selection(a_ref, groups_rows, tokens, start, width):
    named = a_ref[groups_rows:groups_rows + 1, 0:groups_rows].astype(F32)[:, start:start + width]
    return (lax.broadcasted_iota(jnp.int32, (tokens, 1), 0).astype(F32) + 1.0 == named).astype(F32).astype(BF16)


def token_grads_kernel(n, cap, local, *refs):
    a_refs, c_refs = refs[:n], refs[n:2 * n]
    up_refs, down_refs = refs[2 * n:2 * n + 2], refs[2 * n + 2:2 * n + 4]
    outs = refs[2 * n + 4:]
    part_refs, grad_rows_ref, cot_ref, slot_ref = outs[:n], outs[n], outs[n + 1], outs[n + 2]
    groups = 2 * local
    slots = groups * cap
    tokens = c_refs[0].shape[0]
    for k in range(n):
        pick = selection(a_refs[k], slots, tokens, 0, slots)
        rows = dot(pick, c_refs[k][...], TN).astype(BF16)
        for g in range(groups):
            cot_ref[g, k * cap:(k + 1) * cap, :] = rows[g * cap:(g + 1) * cap]
    for g in range(groups):
        grad_hidden = dot(cot_ref[g], down_refs[g // local][g % local], NT)
        act = jnp.concatenate([a_refs[k][g * cap:(g + 1) * cap, :] for k in range(n)], axis=0)
        grad_rows = (grad_hidden * act.astype(F32)).astype(BF16)
        grad_rows_ref[g] = grad_rows
        slot_grad = dot(grad_rows, up_refs[g // local][g % local], NT).astype(BF16)
        for k in range(n):
            slot_ref[k, g * cap:(g + 1) * cap, :] = slot_grad[k * cap:(k + 1) * cap]
    for k in range(n):
        pick = selection(a_refs[k], slots, tokens, 0, slots)
        part_refs[k][...] = dot(pick, slot_ref[k]).astype(BF16)


def token_grads(acts, cots, ups, downs, cap, local):
    n = len(acts)
    tokens, width = cots[0].shape
    hidden = ups[0].shape[2]
    groups = 2 * local
    outs = [jax.ShapeDtypeStruct((tokens, width), BF16)] * n + [
        jax.ShapeDtypeStruct((groups, n * cap, hidden), BF16),
        jax.ShapeDtypeStruct((groups, n * cap, width), BF16),
    ]
    result = pl.pallas_call(
        functools.partial(token_grads_kernel, n, cap, local),
        out_shape=outs,
        scratch_shapes=[pltpu.VMEM((n, groups * cap, width), BF16)],
        name="token_grads",
        compiler_params=pltpu.CompilerParams(vmem_limit_bytes=50 << 20),
        cost_estimate=pl.CostEstimate(
            flops=4 * groups * n * cap * hidden * width, bytes_accessed=24 << 20, transcendentals=0
        ),
    )(*acts, *cots, *ups, *downs)
    return result[:n], result[n], result[n + 1]


def weight_grads_kernel(n, cap, local, pair, added, *refs):
    a_refs, x_refs = refs[:n], refs[n:2 * n]
    up_ref, grad_rows_ref, cot_ref = refs[2 * n:2 * n + 3]
    more = refs[2 * n + 3:2 * n + 3 + 2 * added]
    grad_up_ref, grad_down_ref, x_ref = refs[2 * n + 3 + 2 * added:]
    slots = 2 * local * cap
    tokens = x_refs[0].shape[0]
    for k in range(n):
        pick = selection(a_refs[k], slots, tokens, pair * local * cap, local * cap)
        rows = dot(pick, x_refs[k][...], TN).astype(BF16)
        for j in range(local):
            x_ref[j, k * cap:(k + 1) * cap, :] = rows[j * cap:(j + 1) * cap]
    for j in range(local):
        g = pair * local + j
        act = jnp.concatenate([a_refs[k][g * cap:(g + 1) * cap, :] for k in range(n)], axis=0)
        hidden = (dot(x_ref[j], up_ref[j]) * act.astype(F32)).astype(BF16)
        grad_down = dot(hidden, cot_ref[g], TN)
        grad_up = dot(x_ref[j], grad_rows_ref[g], TN)
        if added:
            grad_up = grad_up + more[0][j].astype(F32)
            grad_down = grad_down + more[1][j].astype(F32)
        grad_down_ref[j] = grad_down.astype(BF16)
        grad_up_ref[j] = grad_up.astype(BF16)


def weight_grads(acts, xs, up, grad_rows, cot_rows, cap, pair, more=()):
    n = len(acts)
    local, width, hidden = up.shape
    return pl.pallas_call(
        functools.partial(weight_grads_kernel, n, cap, local, pair, len(more) // 2),
        out_shape=[
            jax.ShapeDtypeStruct((local, width, hidden), BF16),
            jax.ShapeDtypeStruct((local, hidden, width), BF16),
        ],
        scratch_shapes=[pltpu.VMEM((local, n * cap, width), BF16)],
        name=f"weight_grads_{pair}",
        compiler_params=pltpu.CompilerParams(vmem_limit_bytes=50 << 20),
        cost_estimate=pl.CostEstimate(
            flops=6 * local * n * cap * hidden * width, bytes_accessed=24 << 20, transcendentals=0
        ),
    )(*acts, *xs, up, grad_rows, cot_rows, *more)


def body(inputs, upstream, gate_saved, expert_ids, route_weights, w_up, w_down):
    grid = Grid()
    local = w_up.shape[1]
    experts = local * grid.size
    tokens, top = expert_ids.shape[1:]
    hidden = w_up.shape[3]
    capacity = 3 * tokens * top // (2 * experts)
    cap = -(-capacity // 16) * 16
    zs, xs = grid.z, grid.x
    quads = zs == 4
    z_here = lax.axis_index("ep") // 2 // xs
    inner = (z_here == 1) | (z_here == 2)

    def along_z(d):
        return lambda z, x, core: (z ^ d, x, core)

    def along_x(d):
        return lambda z, x, core: (z, x ^ d, core)

    def across(z, x, core):
        return (z, x, 1 - core)

    def middle(z, x, core):
        return (3 - z, x, core) if z in (1, 2) else None

    def outward(z, x, core):
        return {1: (0, x, core), 2: (3, x, core)}.get(z)

    def inward(z, x, core):
        return {0: (1, x, core), 3: (2, x, core)}.get(z)

    def spread(block):
        rows = [block] + [None] * (zs - 1)
        if quads:
            rows[1] = grid.move(block, along_z(1))
            near = grid.move(block, middle)
            rows[2] = grid.move(block, along_z(2))
            far = grid.move(rows[2], outward)
            rows[3] = jnp.where(inner, near, far)
        else:
            for d in range(1, zs):
                rows[d] = grid.move(block, along_z(d))
        return [row if d == 0 else grid.move(row, along_x(d)) for row in rows for d in range(xs)]

    cotangent = lax.ppermute(
        upstream[0],
        "section",
        [((i + 1) % grid.sections, i) for i in range(grid.sections)],
    )
    tokens_all = spread(inputs[0])

    scale = route_weights[0][:, :, None]
    act = (scale * jax.nn.silu(gate_saved[0].astype(F32))).astype(BF16)
    act = act.reshape(tokens * top, hidden)
    ids_row = expert_ids[0].reshape(1, tokens * top)
    blocks = prep(ids_row, act, top, cap, local, grid.chips)
    acts = [blocks[0]]
    for k in range(1, grid.chips):
        acts.append(grid.move(blocks[k], lambda z, x, core, k=k: (z ^ (k // xs), x ^ (k % xs), core)))

    cots = spread(cotangent)
    ups = (w_up[0], grid.move(w_up[0], across))
    downs = (w_down[0], grid.move(w_down[0], across))
    parts, grad_rows, cot_rows = token_grads(acts, cots, ups, downs, cap, local)

    def total(*values):
        return functools.reduce(jnp.add, [v.astype(F32) for v in values]).astype(BF16)

    rows = [None] * zs
    for z in reversed(range(zs)):
        arrived = [grid.move(parts[z * xs + d], along_x(d)) for d in range(1, xs)]
        rows[z] = total(parts[z * xs], *arrived)
    if quads:
        rows[2] = total(rows[2], grid.move(rows[3], inward))
        last = [
            grid.move(rows[3], middle, -1),
            grid.move(rows[2], along_z(2), -1),
            grid.move(rows[1], along_z(1), -1),
        ]
    else:
        last = [grid.move(rows[d], along_z(d), -1) for d in range(1, zs)]
    last.append(grid.move(rows[0], along_z(0), -1))
    delivered = total(*last)[None]

    theirs = weight_grads(acts, tokens_all, ups[1], grad_rows, cot_rows, cap, 1)
    given = [grid.move(v, across) for v in theirs]
    grad_up, grad_down = weight_grads(acts, tokens_all, ups[0], grad_rows, cot_rows, cap, 0, given)
    return (delivered, grad_up[None], grad_down[None])


def solution(mesh):
    return jax.shard_map(
        body,
        mesh=mesh,
        in_specs=(
            P("section", "ep", None),
            P("section", "ep", None),
            P("section", "ep", None, None),
            P("section", "ep", None),
            P("section", "ep", None),
            P("section", "ep", None, None),
            P("section", "ep", None, None),
        ),
        out_specs=(
            P("section", "ep", None),
            P("section", "ep", None, None),
            P("section", "ep", None, None),
        ),
        check_vma=False,
    )
```

```python
import functools

import jax
import jax.numpy as jnp
from jax import lax
from jax.experimental import pallas as pl
from jax.experimental.pallas import tpu as pltpu
from jax.sharding import PartitionSpec as P


F32 = jnp.float32
BF16 = jnp.bfloat16
EXTRA = 8
NT = (((1,), (1,)), ((), ()))
TN = (((0,), (0,)), ((), ()))


def dot(a, b, dims=(((1,), (0,)), ((), ()))):
    return lax.dot_general(a, b, dims, preferred_element_type=F32)


class Grid:
    def __init__(self):
        self.sections = lax.axis_size("section")
        self.size = lax.axis_size("ep")
        self.chips = self.size // 2
        bits = self.chips.bit_length() - 1
        self.z = 1 << ((bits + 1) // 2)
        self.x = self.chips // self.z

    def move(self, block, target, shift=0):
        pairs = []
        for s in range(self.sections):
            for i in range(self.size):
                to = target(i // 2 // self.x, i // 2 % self.x, i % 2)
                if to is not None:
                    z, x, core = to
                    there = (z * self.x + x) * 2 + core
                    pairs.append((s * self.size + i, (s + shift) % self.sections * self.size + there))
        return lax.ppermute(block, ("section", "ep"), pairs)


def prep_kernel(top, cap, local, ids_ref, act_ref, *out_refs):
    index = lax.axis_index("ep")
    chip, core = index // 2, index % 2
    rows = act_ref.shape[0]
    experts = len(out_refs) * 2 * local
    ids = ids_ref[...]
    named = lax.broadcasted_iota(jnp.int32, (experts, rows), 0) == ids
    upper = lax.broadcasted_iota(jnp.int32, (rows, rows), 0) <= lax.broadcasted_iota(jnp.int32, (rows, rows), 1)
    count = dot(named.astype(F32).astype(BF16), upper.astype(F32).astype(BF16))
    position = jnp.sum(jnp.where(named, count, 0.0), axis=0, keepdims=True).astype(jnp.int32) - 1
    slot = ids * cap + position
    half = local * cap
    place = lax.broadcasted_iota(jnp.int32, (2 * half, 1), 0)
    token = (lax.broadcasted_iota(jnp.int32, (EXTRA, rows), 1) // top + 1).astype(F32).astype(BF16)
    for k, out_ref in enumerate(out_refs):
        first = ((chip ^ k) * 2 + core) * half
        second = ((chip ^ k) * 2 + 1 - core) * half
        mine = jnp.where(place < half, place + first, place - half + second)
        onehot = (mine == slot).astype(F32).astype(BF16)
        out_ref[0:2 * half, :] = dot(onehot, act_ref[...]).astype(BF16)
        out_ref[2 * half:2 * half + EXTRA, :] = jnp.zeros((EXTRA, out_ref.shape[1]), BF16)
        out_ref[2 * half:2 * half + EXTRA, 0:2 * half] = dot(token, onehot, NT).astype(BF16)


def prep(ids_row, act, top, cap, local, chips):
    rows, width = act.shape
    shape = jax.ShapeDtypeStruct((2 * local * cap + EXTRA, width), BF16)
    return pl.pallas_call(
        functools.partial(prep_kernel, top, cap, local),
        out_shape=[shape] * chips,
        name="prep",
        compiler_params=pltpu.CompilerParams(vmem_limit_bytes=24 << 20),
        cost_estimate=pl.CostEstimate(
            flops=4 * rows * rows * width, bytes_accessed=4 * rows * width, transcendentals=0
        ),
    )(ids_row, act)


def selection(a_ref, groups_rows, tokens, start, width):
    named = a_ref[groups_rows:groups_rows + 1, 0:groups_rows].astype(F32)[:, start:start + width]
    return (lax.broadcasted_iota(jnp.int32, (tokens, 1), 0).astype(F32) + 1.0 == named).astype(F32).astype(BF16)


def token_grads_kernel(n, cap, local, *refs):
    a_refs, c_refs = refs[:n], refs[n:2 * n]
    up_refs, down_refs = refs[2 * n:2 * n + 2], refs[2 * n + 2:2 * n + 4]
    outs = refs[2 * n + 4:]
    part_refs, grad_rows_ref, cot_ref, slot_ref = outs[:n], outs[n], outs[n + 1], outs[n + 2]
    groups = 2 * local
    slots = groups * cap
    tokens = c_refs[0].shape[0]
    for k in range(n):
        pick = selection(a_refs[k], slots, tokens, 0, slots)
        rows = dot(pick, c_refs[k][...], TN).astype(BF16)
        for g in range(groups):
            cot_ref[g, k * cap:(k + 1) * cap, :] = rows[g * cap:(g + 1) * cap]
    for g in range(groups):
        grad_hidden = dot(cot_ref[g], down_refs[g // local][g % local], NT)
        act = jnp.concatenate([a_refs[k][g * cap:(g + 1) * cap, :] for k in range(n)], axis=0)
        grad_rows = (grad_hidden * act.astype(F32)).astype(BF16)
        grad_rows_ref[g] = grad_rows
        slot_grad = dot(grad_rows, up_refs[g // local][g % local], NT).astype(BF16)
        for k in range(n):
            slot_ref[k, g * cap:(g + 1) * cap, :] = slot_grad[k * cap:(k + 1) * cap]
    for k in range(n):
        pick = selection(a_refs[k], slots, tokens, 0, slots)
        part_refs[k][...] = dot(pick, slot_ref[k]).astype(BF16)


def token_grads(acts, cots, ups, downs, cap, local):
    n = len(acts)
    tokens, width = cots[0].shape
    hidden = ups[0].shape[2]
    groups = 2 * local
    outs = [jax.ShapeDtypeStruct((tokens, width), BF16)] * n + [
        jax.ShapeDtypeStruct((groups, n * cap, hidden), BF16),
        jax.ShapeDtypeStruct((groups, n * cap, width), BF16),
    ]
    result = pl.pallas_call(
        functools.partial(token_grads_kernel, n, cap, local),
        out_shape=outs,
        scratch_shapes=[pltpu.VMEM((n, groups * cap, width), BF16)],
        name="token_grads",
        compiler_params=pltpu.CompilerParams(vmem_limit_bytes=36 << 20),
        cost_estimate=pl.CostEstimate(
            flops=4 * groups * n * cap * hidden * width, bytes_accessed=24 << 20, transcendentals=0
        ),
    )(*acts, *cots, *ups, *downs)
    return result[:n], result[n], result[n + 1]


def weight_grads_kernel(n, cap, groups, group, added, *refs):
    a_refs, x_refs = refs[:n], refs[n:2 * n]
    up_ref, grad_rows_ref, cot_ref = refs[2 * n:2 * n + 3]
    more = refs[2 * n + 3:2 * n + 3 + 2 * added]
    grad_up_ref, grad_down_ref, x_ref = refs[-3:]
    tokens = x_refs[0].shape[0]
    for k in range(n):
        pick = selection(a_refs[k], groups * cap, tokens, group * cap, cap)
        x_ref[k * cap:(k + 1) * cap, :] = dot(pick, x_refs[k][...], TN).astype(BF16)
    act = jnp.concatenate([a_refs[k][group * cap:(group + 1) * cap, :] for k in range(n)], axis=0)
    hidden = (dot(x_ref[...], up_ref[0]) * act.astype(F32)).astype(BF16)
    grad_down = dot(hidden, cot_ref[0], TN)
    grad_up = dot(x_ref[...], grad_rows_ref[0], TN)
    if added:
        grad_up = grad_up + more[0][0].astype(F32)
        grad_down = grad_down + more[1][0].astype(F32)
    grad_down_ref[0] = grad_down.astype(BF16)
    grad_up_ref[0] = grad_up.astype(BF16)


def weight_grads(acts, xs, up, grad_rows, cot_rows, cap, group, more=(), total=1, into=()):
    n = len(acts)
    local, width, hidden = up.shape
    rows = n * cap
    mine = group if total > 1 else 0

    def whole(v):
        return pl.BlockSpec(v.shape, lambda i: (0,) * v.ndim)

    def one(v, j):
        return pl.BlockSpec((1, *v.shape[1:]), lambda i: (j, 0, 0))

    outs = [
        jax.ShapeDtypeStruct((total, width, hidden), BF16),
        jax.ShapeDtypeStruct((total, hidden, width), BF16),
    ]
    operands = (*acts, *xs, up, grad_rows, cot_rows, *more, *into)
    first = len(operands) - len(into)
    return pl.pallas_call(
        functools.partial(weight_grads_kernel, n, cap, 2 * local, group, len(more) // 2),
        grid=(1,),
        in_specs=[
            *[whole(v) for v in (*acts, *xs)],
            one(up, group % local),
            one(grad_rows, group),
            one(cot_rows, group),
            *[whole(v) for v in more],
            *[pl.BlockSpec(memory_space=pl.ANY) for _ in into],
        ],
        out_specs=[one(v, mine) for v in outs],
        out_shape=outs,
        input_output_aliases={first + i: i for i in range(len(into))},
        scratch_shapes=[pltpu.VMEM((rows, width), BF16)],
        compiler_params=pltpu.CompilerParams(vmem_limit_bytes=32 << 20),
        cost_estimate=pl.CostEstimate(
            flops=6 * rows * hidden * width, bytes_accessed=12 << 20, transcendentals=0
        ),
    )(*operands)


def body(inputs, upstream, gate_saved, expert_ids, route_weights, w_up, w_down):
    grid = Grid()
    local = w_up.shape[1]
    experts = local * grid.size
    tokens, top = expert_ids.shape[1:]
    hidden = w_up.shape[3]
    capacity = 3 * tokens * top // (2 * experts)
    cap = -(-capacity // 16) * 16
    zs, xs = grid.z, grid.x
    quads = zs == 4
    z_here = lax.axis_index("ep") // 2 // xs
    inner = (z_here == 1) | (z_here == 2)

    def along_z(d):
        return lambda z, x, core: (z ^ d, x, core)

    def along_x(d):
        return lambda z, x, core: (z, x ^ d, core)

    def across(z, x, core):
        return (z, x, 1 - core)

    def middle(z, x, core):
        return (3 - z, x, core) if z in (1, 2) else None

    def outward(z, x, core):
        return {1: (0, x, core), 2: (3, x, core)}.get(z)

    def inward(z, x, core):
        return {0: (1, x, core), 3: (2, x, core)}.get(z)

    def spread(block, far_block=None, side=False):
        rows = [block] + [None] * (zs - 1)
        if quads:
            rows[1] = grid.move(block, along_z(1))
            near = grid.move(block, middle)
            rows[2] = grid.move(block, along_z(2)) if far_block is None else far_block
            far = grid.move(rows[2], outward)
            rows[3] = jnp.where(inner, near, far)
        else:
            for d in range(1, zs):
                rows[d] = grid.move(block, along_z(d))
        blocks = []
        for z, row in enumerate(rows):
            blocks.append(row)
            for d in range(1, xs):
                if side and z == 1:
                    blocks.append(grid.move(blocks[d], along_z(1)))
                else:
                    blocks.append(grid.move(row, along_x(d)))
        return blocks

    cotangent = grid.move(upstream[0], along_z(0), -1)
    cot_far = grid.move(upstream[0], along_z(2), -1) if quads else None
    tokens_all = spread(inputs[0])

    scale = route_weights[0][:, :, None]
    act = (scale * jax.nn.silu(gate_saved[0].astype(F32))).astype(BF16)
    act = act.reshape(tokens * top, hidden)
    ids_row = expert_ids[0].reshape(1, tokens * top)
    blocks = prep(ids_row, act, top, cap, local, grid.chips)
    acts = [blocks[0]]
    for k in range(1, grid.chips):
        acts.append(grid.move(blocks[k], lambda z, x, core, k=k: (z ^ (k // xs), x ^ (k % xs), core)))

    cots = spread(cotangent, cot_far, quads)
    ups = (w_up[0], grid.move(w_up[0], across))
    downs = (w_down[0], grid.move(w_down[0], across))
    parts, grad_rows, cot_rows = token_grads(acts, cots, ups, downs, cap, local)

    def total(*values):
        return functools.reduce(jnp.add, [v.astype(F32) for v in values]).astype(BF16)

    rows = [None] * zs
    parts = list(parts)
    if quads:
        rows[1] = parts[xs]
        for d in range(1, xs):
            parts[d] = total(parts[d], grid.move(parts[xs + d], along_z(1)))
    for z in reversed(range(zs)):
        if rows[z] is None:
            arrived = [grid.move(parts[z * xs + d], along_x(d)) for d in range(1, xs)]
            rows[z] = total(parts[z * xs], *arrived)
    if quads:
        rows[2] = total(rows[2], grid.move(rows[3], inward))
        last = [grid.move(rows[3], middle, -1), grid.move(rows[2], along_z(2), -1), grid.move(rows[1], along_z(1), -1)]
    else:
        last = [grid.move(rows[d], along_z(d), -1) for d in range(1, zs)]
    last.append(grid.move(rows[0], along_z(0), -1))
    delivered = total(*last)[None]

    given = []
    for j in range(local):
        theirs = weight_grads(acts, tokens_all, ups[1], grad_rows, cot_rows, cap, local + j)
        given.append([grid.move(theirs[0], across), grid.move(theirs[1], across)])
    ours = ()
    for j in range(local):
        ours = weight_grads(acts, tokens_all, ups[0], grad_rows, cot_rows, cap, j, given[j], local, ours)
    grad_up, grad_down = ours
    return (delivered, grad_up[None], grad_down[None])


def solution(mesh):
    return jax.shard_map(
        body,
        mesh=mesh,
        in_specs=(
            P("section", "ep", None),
            P("section", "ep", None),
            P("section", "ep", None, None),
            P("section", "ep", None),
            P("section", "ep", None),
            P("section", "ep", None, None),
            P("section", "ep", None, None),
        ),
        out_specs=(
            P("section", "ep", None),
            P("section", "ep", None, None),
            P("section", "ep", None, None),
        ),
        check_vma=False,
    )
```

```python
import functools

import jax
import jax.numpy as jnp
from jax import lax
from jax.experimental import pallas as pl
from jax.experimental.pallas import tpu as pltpu
from jax.sharding import PartitionSpec as P


F32 = jnp.float32
BF16 = jnp.bfloat16
EXTRA = 8
NT = (((1,), (1,)), ((), ()))
TN = (((0,), (0,)), ((), ()))


def dot(a, b, dims=(((1,), (0,)), ((), ()))):
    return lax.dot_general(a, b, dims, preferred_element_type=F32)


class Grid:
    def __init__(self):
        self.sections = lax.axis_size("section")
        self.size = lax.axis_size("ep")
        self.chips = self.size // 2
        bits = self.chips.bit_length() - 1
        self.z = 1 << ((bits + 1) // 2)
        self.x = self.chips // self.z

    def move(self, block, target, shift=0):
        pairs = []
        for s in range(self.sections):
            for i in range(self.size):
                to = target(i // 2 // self.x, i // 2 % self.x, i % 2)
                if to is not None:
                    z, x, core = to
                    there = (z * self.x + x) * 2 + core
                    pairs.append((s * self.size + i, (s + shift) % self.sections * self.size + there))
        return lax.ppermute(block, ("section", "ep"), pairs)


def prep_kernel(top, cap, local, ids_ref, act_ref, *out_refs):
    index = lax.axis_index("ep")
    chip, core = index // 2, index % 2
    rows = act_ref.shape[0]
    experts = len(out_refs) * 2 * local
    ids = ids_ref[...]
    named = lax.broadcasted_iota(jnp.int32, (experts, rows), 0) == ids
    upper = lax.broadcasted_iota(jnp.int32, (rows, rows), 0) <= lax.broadcasted_iota(jnp.int32, (rows, rows), 1)
    count = dot(named.astype(F32).astype(BF16), upper.astype(F32).astype(BF16))
    position = jnp.sum(jnp.where(named, count, 0.0), axis=0, keepdims=True).astype(jnp.int32) - 1
    slot = ids * cap + position
    half = local * cap
    place = lax.broadcasted_iota(jnp.int32, (2 * half, 1), 0)
    token = (lax.broadcasted_iota(jnp.int32, (EXTRA, rows), 1) // top + 1).astype(F32).astype(BF16)
    for k, out_ref in enumerate(out_refs):
        first = ((chip ^ k) * 2 + core) * half
        second = ((chip ^ k) * 2 + 1 - core) * half
        mine = jnp.where(place < half, place + first, place - half + second)
        onehot = (mine == slot).astype(F32).astype(BF16)
        out_ref[0:2 * half, :] = dot(onehot, act_ref[...]).astype(BF16)
        out_ref[2 * half:2 * half + EXTRA, :] = jnp.zeros((EXTRA, out_ref.shape[1]), BF16)
        out_ref[2 * half:2 * half + EXTRA, 0:2 * half] = dot(token, onehot, NT).astype(BF16)


def prep(ids_row, act, top, cap, local, chips):
    rows, width = act.shape
    shape = jax.ShapeDtypeStruct((2 * local * cap + EXTRA, width), BF16)
    return pl.pallas_call(
        functools.partial(prep_kernel, top, cap, local),
        out_shape=[shape] * chips,
        name="prep",
        compiler_params=pltpu.CompilerParams(vmem_limit_bytes=24 << 20),
        cost_estimate=pl.CostEstimate(
            flops=4 * rows * rows * width, bytes_accessed=4 * rows * width, transcendentals=0
        ),
    )(ids_row, act)


def selection(a_ref, groups_rows, tokens, start, width):
    named = a_ref[groups_rows:groups_rows + 1, 0:groups_rows].astype(F32)[:, start:start + width]
    return (lax.broadcasted_iota(jnp.int32, (tokens, 1), 0).astype(F32) + 1.0 == named).astype(F32).astype(BF16)


def token_grads_kernel(n, cap, local, *refs):
    a_refs, c_refs = refs[:n], refs[n:2 * n]
    up_refs, down_refs = refs[2 * n:2 * n + 2], refs[2 * n + 2:2 * n + 4]
    outs = refs[2 * n + 4:]
    part_refs, grad_rows_ref, cot_ref, slot_ref = outs[:n], outs[n], outs[n + 1], outs[n + 2]
    groups = 2 * local
    slots = groups * cap
    tokens = c_refs[0].shape[0]
    for k in range(n):
        pick = selection(a_refs[k], slots, tokens, 0, slots)
        rows = dot(pick, c_refs[k][...], TN).astype(BF16)
        for g in range(groups):
            cot_ref[g, k * cap:(k + 1) * cap, :] = rows[g * cap:(g + 1) * cap]
    for g in range(groups):
        grad_hidden = dot(cot_ref[g], down_refs[g // local][g % local], NT)
        act = jnp.concatenate([a_refs[k][g * cap:(g + 1) * cap, :] for k in range(n)], axis=0)
        grad_rows = (grad_hidden * act.astype(F32)).astype(BF16)
        grad_rows_ref[g] = grad_rows
        slot_grad = dot(grad_rows, up_refs[g // local][g % local], NT).astype(BF16)
        for k in range(n):
            slot_ref[k, g * cap:(g + 1) * cap, :] = slot_grad[k * cap:(k + 1) * cap]
    for k in range(n):
        pick = selection(a_refs[k], slots, tokens, 0, slots)
        part_refs[k][...] = dot(pick, slot_ref[k]).astype(BF16)


def token_grads(acts, cots, ups, downs, cap, local):
    n = len(acts)
    tokens, width = cots[0].shape
    hidden = ups[0].shape[2]
    groups = 2 * local
    outs = [jax.ShapeDtypeStruct((tokens, width), BF16)] * n + [
        jax.ShapeDtypeStruct((groups, n * cap, hidden), BF16),
        jax.ShapeDtypeStruct((groups, n * cap, width), BF16),
    ]
    result = pl.pallas_call(
        functools.partial(token_grads_kernel, n, cap, local),
        out_shape=outs,
        scratch_shapes=[pltpu.VMEM((n, groups * cap, width), BF16)],
        name="token_grads",
        compiler_params=pltpu.CompilerParams(vmem_limit_bytes=26 << 20),
        cost_estimate=pl.CostEstimate(
            flops=4 * groups * n * cap * hidden * width, bytes_accessed=24 << 20, transcendentals=0
        ),
    )(*acts, *cots, *ups, *downs)
    return result[:n], result[n], result[n + 1]


def gather_kernel(n, cap, groups, *refs):
    a_refs, x_refs, out_ref = refs[:n], refs[n:2 * n], refs[2 * n]
    tokens = x_refs[0].shape[0]
    for k in range(n):
        pick = selection(a_refs[k], groups * cap, tokens, 0, groups * cap)
        rows = dot(pick, x_refs[k][...], TN).astype(BF16)
        for g in range(groups):
            out_ref[g, k * cap:(k + 1) * cap, :] = rows[g * cap:(g + 1) * cap]


def gather(acts, xs, cap, groups):
    n = len(acts)
    width = xs[0].shape[1]
    return pl.pallas_call(
        functools.partial(gather_kernel, n, cap, groups),
        out_shape=jax.ShapeDtypeStruct((groups, n * cap, width), BF16),
        name="gather",
        compiler_params=pltpu.CompilerParams(vmem_limit_bytes=20 << 20),
        cost_estimate=pl.CostEstimate(
            flops=2 * n * groups * cap * width * xs[0].shape[0], bytes_accessed=4 << 20, transcendentals=0
        ),
    )(*acts, *xs)


def weight_grads_kernel(n, cap, first, added, *refs):
    a_refs, (x_ref, up_ref, grad_rows_ref, cot_ref), more = refs[:n], refs[n:n + 4], refs[n + 4:n + 4 + 2 * added]
    grad_up_ref, grad_down_ref = refs[-2:]
    rows = pl.ds(pl.multiple_of((first + pl.program_id(0)) * cap, cap), cap)
    act = jnp.concatenate([a_ref[rows, :] for a_ref in a_refs], axis=0)
    hidden = (dot(x_ref[0], up_ref[0]) * act.astype(F32)).astype(BF16)
    grad_down = dot(hidden, cot_ref[0], TN)
    grad_up = dot(x_ref[0], grad_rows_ref[0], TN)
    for i in range(added):
        grad_up = grad_up + more[2 * i][0].astype(F32)
        grad_down = grad_down + more[2 * i + 1][0].astype(F32)
    grad_down_ref[0] = grad_down.astype(BF16)
    grad_up_ref[0] = grad_up.astype(BF16)


def weight_grads(acts, x_rows, up, grad_rows, cot_rows, cap, group, count, more=(), total=None, into=()):
    n = len(acts)
    local, width, hidden = up.shape
    at = 0 if total is None else group % local
    total = count if total is None else total

    def whole(v):
        return pl.BlockSpec(v.shape, lambda i: (0,) * v.ndim)

    def from_(v, j):
        return pl.BlockSpec((1, *v.shape[1:]), lambda i: (j + i, 0, 0))

    outs = [
        jax.ShapeDtypeStruct((total, width, hidden), BF16),
        jax.ShapeDtypeStruct((total, hidden, width), BF16),
    ]
    added = [(v, j) for pair, j in more for v in pair]
    operands = (*acts, x_rows, up, grad_rows, cot_rows, *[v for v, _ in added], *into)
    before = len(operands) - len(into)
    return pl.pallas_call(
        functools.partial(weight_grads_kernel, n, cap, group, len(more)),
        grid=(count,),
        in_specs=[
            *[whole(v) for v in acts],
            from_(x_rows, group),
            from_(up, group % local),
            from_(grad_rows, group),
            from_(cot_rows, group),
            *[from_(v, j) for v, j in added],
            *[pl.BlockSpec(memory_space=pl.ANY) for _ in into],
        ],
        out_specs=[from_(v, at) for v in outs],
        out_shape=outs,
        input_output_aliases={before + i: i for i in range(len(into))},
        compiler_params=pltpu.CompilerParams(vmem_limit_bytes=20 << 20),
        cost_estimate=pl.CostEstimate(
            flops=6 * count * n * cap * hidden * width, bytes_accessed=count * (8 << 20), transcendentals=0
        ),
    )(*operands)


def body(inputs, upstream, gate_saved, expert_ids, route_weights, w_up, w_down):
    grid = Grid()
    local = w_up.shape[1]
    experts = local * grid.size
    tokens, top = expert_ids.shape[1:]
    hidden = w_up.shape[3]
    capacity = 3 * tokens * top // (2 * experts)
    cap = -(-capacity // 16) * 16
    zs, xs = grid.z, grid.x
    quads = zs == 4
    z_here = lax.axis_index("ep") // 2 // xs
    inner = (z_here == 1) | (z_here == 2)

    def along_z(d):
        return lambda z, x, core: (z ^ d, x, core)

    def along_x(d):
        return lambda z, x, core: (z, x ^ d, core)

    def across(z, x, core):
        return (z, x, 1 - core)

    def middle(z, x, core):
        return (3 - z, x, core) if z in (1, 2) else None

    def outward(z, x, core):
        return {1: (0, x, core), 2: (3, x, core)}.get(z)

    def inward(z, x, core):
        return {0: (1, x, core), 3: (2, x, core)}.get(z)

    def spread(block, side=False):
        rows = [block] + [None] * (zs - 1)
        if quads:
            rows[1] = grid.move(block, along_z(1))
            near = grid.move(block, middle)
            on = grid.move(rows[1], middle)
            out1 = grid.move(near, outward)
            out2 = grid.move(on, outward)
            rows[2] = jnp.where(inner, on, out1)
            rows[3] = jnp.where(inner, near, out2)
        else:
            for d in range(1, zs):
                rows[d] = grid.move(block, along_z(d))
        blocks = []
        for z, row in enumerate(rows):
            blocks.append(row)
            for d in range(1, xs):
                if side and z == 1:
                    blocks.append(grid.move(blocks[d], along_z(1)))
                else:
                    blocks.append(grid.move(row, along_x(d)))
        return blocks

    cotangent = grid.move(upstream[0], along_z(0), -1)
    tokens_all = spread(inputs[0])

    scale = route_weights[0][:, :, None]
    act = (scale * jax.nn.silu(gate_saved[0].astype(F32))).astype(BF16)
    act = act.reshape(tokens * top, hidden)
    ids_row = expert_ids[0].reshape(1, tokens * top)
    blocks = prep(ids_row, act, top, cap, local, grid.chips)
    acts = [blocks[0]]
    for k in range(1, grid.chips):
        acts.append(grid.move(blocks[k], lambda z, x, core, k=k: (z ^ (k // xs), x ^ (k % xs), core)))

    cots = spread(cotangent, quads)
    ups = (w_up[0], grid.move(w_up[0], across))
    downs = (w_down[0], grid.move(w_down[0], across))
    groups = 2 * local
    split = zs // 2 * xs
    halves = (range(split), range(split, grid.chips))
    parts, grad_rows, cot_rows = [None] * grid.chips, [], []
    for members in halves:
        some, rows, cot = token_grads([acts[k] for k in members], [cots[k] for k in members], ups, downs, cap, local)
        grad_rows.append(rows)
        cot_rows.append(cot)
        for k, part in zip(members, some):
            parts[k] = part

    def total(*values):
        return functools.reduce(jnp.add, [v.astype(F32) for v in values]).astype(BF16)

    rows = [None] * zs
    if quads:
        rows[1] = parts[xs]
        for d in range(1, xs):
            parts[d] = total(parts[d], grid.move(parts[xs + d], along_z(1)))
    for z in reversed(range(zs)):
        if rows[z] is None:
            arrived = [grid.move(parts[z * xs + d], along_x(d)) for d in range(1, xs)]
            rows[z] = total(parts[z * xs], *arrived)
    if quads:
        rows[2] = total(rows[2], grid.move(rows[3], inward))
        last = [grid.move(rows[3], middle, -1), grid.move(rows[2], along_z(2), -1), grid.move(rows[1], along_z(1), -1)]
    else:
        last = [grid.move(rows[d], along_z(d), -1) for d in range(1, zs)]
    last.append(grid.move(rows[0], along_z(0), -1))
    delivered = total(*last)[None]

    x_rows = []
    for members in halves:
        x_rows.append(gather([acts[k] for k in members], [tokens_all[k] for k in members], cap, groups))
    sides = []
    for h, members in enumerate(halves):
        sides.append(([acts[k] for k in members], x_rows[h]))
    near_half = []
    for p in range(2):
        near_half.append(weight_grads(*sides[0], ups[p], grad_rows[0], cot_rows[0], cap, p * local, local))
    far_half = (*sides[1],)
    given = []
    for j in range(local):
        theirs = weight_grads(*far_half, ups[1], grad_rows[1], cot_rows[1], cap, local + j, 1, [(near_half[1], j)])
        given.append([grid.move(theirs[0], across), grid.move(theirs[1], across)])
    ours = ()
    for j in range(local):
        more = [(near_half[0], j), (given[j], 0)]
        ours = weight_grads(*far_half, ups[0], grad_rows[1], cot_rows[1], cap, j, 1, more, local, ours)
    grad_up, grad_down = ours
    return (delivered, grad_up[None], grad_down[None])


def solution(mesh):
    return jax.shard_map(
        body,
        mesh=mesh,
        in_specs=(
            P("section", "ep", None),
            P("section", "ep", None),
            P("section", "ep", None, None),
            P("section", "ep", None),
            P("section", "ep", None),
            P("section", "ep", None, None),
            P("section", "ep", None, None),
        ),
        out_specs=(
            P("section", "ep", None),
            P("section", "ep", None, None),
            P("section", "ep", None, None),
        ),
        check_vma=False,
    )
```

```python
import functools

import jax
import jax.numpy as jnp
from jax import lax
from jax.experimental import pallas as pl
from jax.experimental.pallas import tpu as pltpu
from jax.sharding import PartitionSpec as P


F32 = jnp.float32
BF16 = jnp.bfloat16
EXTRA = 8
NT = (((1,), (1,)), ((), ()))
TN = (((0,), (0,)), ((), ()))


def dot(a, b, dims=(((1,), (0,)), ((), ()))):
    return lax.dot_general(a, b, dims, preferred_element_type=F32)


class Grid:
    def __init__(self):
        self.sections = lax.axis_size("section")
        self.size = lax.axis_size("ep")
        self.chips = self.size // 2
        bits = self.chips.bit_length() - 1
        self.z = 1 << ((bits + 1) // 2)
        self.x = self.chips // self.z

    def move(self, block, target, shift=0):
        pairs = []
        for s in range(self.sections):
            for i in range(self.size):
                to = target(i // 2 // self.x, i // 2 % self.x, i % 2)
                if to is not None:
                    z, x, core = to
                    there = (z * self.x + x) * 2 + core
                    pairs.append((s * self.size + i, (s + shift) % self.sections * self.size + there))
        return lax.ppermute(block, ("section", "ep"), pairs)


def prep_kernel(top, cap, local, ids_ref, act_ref, *out_refs):
    index = lax.axis_index("ep")
    chip, core = index // 2, index % 2
    rows = act_ref.shape[0]
    experts = len(out_refs) * 2 * local
    ids = ids_ref[...]
    named = lax.broadcasted_iota(jnp.int32, (experts, rows), 0) == ids
    upper = lax.broadcasted_iota(jnp.int32, (rows, rows), 0) <= lax.broadcasted_iota(jnp.int32, (rows, rows), 1)
    count = dot(named.astype(F32).astype(BF16), upper.astype(F32).astype(BF16))
    position = jnp.sum(jnp.where(named, count, 0.0), axis=0, keepdims=True).astype(jnp.int32) - 1
    slot = ids * cap + position
    half = local * cap
    place = lax.broadcasted_iota(jnp.int32, (2 * half, 1), 0)
    token = (lax.broadcasted_iota(jnp.int32, (EXTRA, rows), 1) // top + 1).astype(F32).astype(BF16)
    for k, out_ref in enumerate(out_refs):
        first = ((chip ^ k) * 2 + core) * half
        second = ((chip ^ k) * 2 + 1 - core) * half
        mine = jnp.where(place < half, place + first, place - half + second)
        onehot = (mine == slot).astype(F32).astype(BF16)
        out_ref[0:2 * half, :] = dot(onehot, act_ref[...]).astype(BF16)
        out_ref[2 * half:2 * half + EXTRA, :] = jnp.zeros((EXTRA, out_ref.shape[1]), BF16)
        out_ref[2 * half:2 * half + EXTRA, 0:2 * half] = dot(token, onehot, NT).astype(BF16)


def prep(ids_row, act, top, cap, local, chips):
    rows, width = act.shape
    shape = jax.ShapeDtypeStruct((2 * local * cap + EXTRA, width), BF16)
    return pl.pallas_call(
        functools.partial(prep_kernel, top, cap, local),
        out_shape=[shape] * chips,
        name="prep",
        compiler_params=pltpu.CompilerParams(vmem_limit_bytes=24 << 20),
        cost_estimate=pl.CostEstimate(
            flops=4 * rows * rows * width, bytes_accessed=4 * rows * width, transcendentals=0
        ),
    )(ids_row, act)


def selection(a_ref, groups_rows, tokens, start, width):
    named = a_ref[groups_rows:groups_rows + 1, 0:groups_rows].astype(F32)[:, start:start + width]
    return (lax.broadcasted_iota(jnp.int32, (tokens, 1), 0).astype(F32) + 1.0 == named).astype(F32).astype(BF16)


def token_grads_kernel(n, cap, local, *refs):
    a_refs, c_refs = refs[:n], refs[n:2 * n]
    up_refs, down_refs = refs[2 * n:2 * n + 2], refs[2 * n + 2:2 * n + 4]
    outs = refs[2 * n + 4:]
    part_refs, (grad_rows_ref, cot_ref, act_ref, slot_ref) = outs[:n], outs[n:]
    groups = 2 * local
    slots = groups * cap
    tokens = c_refs[0].shape[0]
    for k in range(n):
        pick = selection(a_refs[k], slots, tokens, 0, slots)
        rows = dot(pick, c_refs[k][...], TN).astype(BF16)
        for g in range(groups):
            cot_ref[g, k * cap:(k + 1) * cap, :] = rows[g * cap:(g + 1) * cap]
    for g in range(groups):
        grad_hidden = dot(cot_ref[g], down_refs[g // local][g % local], NT)
        act = jnp.concatenate([a_refs[k][g * cap:(g + 1) * cap, :] for k in range(n)], axis=0)
        act_ref[g] = act
        grad_rows = (grad_hidden * act.astype(F32)).astype(BF16)
        grad_rows_ref[g] = grad_rows
        slot_grad = dot(grad_rows, up_refs[g // local][g % local], NT).astype(BF16)
        for k in range(n):
            slot_ref[k, g * cap:(g + 1) * cap, :] = slot_grad[k * cap:(k + 1) * cap]
    for k in range(n):
        pick = selection(a_refs[k], slots, tokens, 0, slots)
        part_refs[k][...] = dot(pick, slot_ref[k]).astype(BF16)


def token_grads(acts, cots, ups, downs, cap, local):
    n = len(acts)
    tokens, width = cots[0].shape
    hidden = ups[0].shape[2]
    groups = 2 * local
    outs = [jax.ShapeDtypeStruct((tokens, width), BF16)] * n + [
        jax.ShapeDtypeStruct((groups, n * cap, hidden), BF16),
        jax.ShapeDtypeStruct((groups, n * cap, width), BF16),
        jax.ShapeDtypeStruct((groups, n * cap, hidden), BF16),
    ]
    result = pl.pallas_call(
        functools.partial(token_grads_kernel, n, cap, local),
        out_shape=outs,
        scratch_shapes=[pltpu.VMEM((n, groups * cap, width), BF16)],
        name="token_grads",
        compiler_params=pltpu.CompilerParams(vmem_limit_bytes=26 << 20),
        cost_estimate=pl.CostEstimate(
            flops=4 * groups * n * cap * hidden * width, bytes_accessed=24 << 20, transcendentals=0
        ),
    )(*acts, *cots, *ups, *downs)
    return result[:n], result[n:]


def gather_kernel(n, cap, groups, *refs):
    a_refs, x_refs, out_refs = refs[:n], refs[n:2 * n], refs[2 * n:]
    tokens = x_refs[0].shape[0]
    local = groups // 2
    for k in range(n):
        pick = selection(a_refs[k], groups * cap, tokens, 0, groups * cap)
        rows = dot(pick, x_refs[k][...], TN).astype(BF16)
        for g in range(groups):
            out_refs[g // local][g % local, k * cap:(k + 1) * cap, :] = rows[g * cap:(g + 1) * cap]


def gather(acts, xs, cap, groups):
    n = len(acts)
    width = xs[0].shape[1]
    return pl.pallas_call(
        functools.partial(gather_kernel, n, cap, groups),
        out_shape=[jax.ShapeDtypeStruct((groups // 2, n * cap, width), BF16)] * 2,
        name="gather",
        compiler_params=pltpu.CompilerParams(vmem_limit_bytes=20 << 20),
        cost_estimate=pl.CostEstimate(
            flops=2 * n * groups * cap * width * xs[0].shape[0], bytes_accessed=4 << 20, transcendentals=0
        ),
    )(*acts, *xs)


def weight_grads_kernel(sets, *refs):
    x, act, grad_rows, cot = [
        jnp.concatenate([refs[4 * i + j][0] for i in range(sets)], axis=0) for j in range(4)
    ]
    up_ref, *more = refs[4 * sets:-2]
    grad_up_ref, grad_down_ref = refs[-2:]
    hidden = (dot(x, up_ref[0]) * act.astype(F32)).astype(BF16)
    grad_down = dot(hidden, cot, TN)
    grad_up = dot(x, grad_rows, TN)
    for i in range(0, len(more), 2):
        grad_up = grad_up + more[i][0].astype(F32)
        grad_down = grad_down + more[i + 1][0].astype(F32)
    grad_down_ref[0] = grad_down.astype(BF16)
    grad_up_ref[0] = grad_up.astype(BF16)


def weight_grads(sets, up, more=()):
    local, width, hidden = up.shape
    operands = [pair for one_set in sets for pair in one_set] + [(up, 0)] + [(v, 0) for v in more]

    def from_(v, j):
        return pl.BlockSpec((1, *v.shape[1:]), lambda i: (j + i, 0, 0))

    outs = [
        jax.ShapeDtypeStruct((local, width, hidden), BF16),
        jax.ShapeDtypeStruct((local, hidden, width), BF16),
    ]
    rows = sum(one_set[0][0].shape[1] for one_set in sets)
    return pl.pallas_call(
        functools.partial(weight_grads_kernel, len(sets)),
        grid=(local,),
        in_specs=[from_(v, j) for v, j in operands],
        out_specs=[from_(v, 0) for v in outs],
        out_shape=outs,
        compiler_params=pltpu.CompilerParams(vmem_limit_bytes=28 << 20),
        cost_estimate=pl.CostEstimate(
            flops=6 * local * rows * hidden * width, bytes_accessed=local * (8 << 20), transcendentals=0
        ),
    )(*[v for v, _ in operands])


def body(inputs, upstream, gate_saved, expert_ids, route_weights, w_up, w_down):
    grid = Grid()
    local = w_up.shape[1]
    experts = local * grid.size
    tokens, top = expert_ids.shape[1:]
    hidden = w_up.shape[3]
    capacity = 3 * tokens * top // (2 * experts)
    cap = -(-capacity // 16) * 16
    zs, xs = grid.z, grid.x
    quads = zs == 4
    z_here = lax.axis_index("ep") // 2 // xs
    inner = (z_here == 1) | (z_here == 2)

    def along_z(d):
        return lambda z, x, core: (z ^ d, x, core)

    def along_x(d):
        return lambda z, x, core: (z, x ^ d, core)

    def across(z, x, core):
        return (z, x, 1 - core)

    def middle(z, x, core):
        return (3 - z, x, core) if z in (1, 2) else None

    def outward(z, x, core):
        return {1: (0, x, core), 2: (3, x, core)}.get(z)

    def inward(z, x, core):
        return {0: (1, x, core), 3: (2, x, core)}.get(z)

    def spread(block, side=False):
        rows = [block] + [None] * (zs - 1)
        if quads:
            rows[1] = grid.move(block, along_z(1))
            near = grid.move(block, middle)
            on = grid.move(rows[1], middle)
            out1 = grid.move(near, outward)
            out2 = grid.move(on, outward)
            rows[2] = jnp.where(inner, on, out1)
            rows[3] = jnp.where(inner, near, out2)
        else:
            for d in range(1, zs):
                rows[d] = grid.move(block, along_z(d))
        blocks = []
        for z, row in enumerate(rows):
            blocks.append(row)
            for d in range(1, xs):
                if side and z == 1:
                    blocks.append(grid.move(blocks[d], along_z(1)))
                else:
                    blocks.append(grid.move(row, along_x(d)))
        return blocks

    cotangent = grid.move(upstream[0], along_z(0), -1)
    tokens_all = spread(inputs[0])

    scale = route_weights[0][:, :, None]
    act = (scale * jax.nn.silu(gate_saved[0].astype(F32))).astype(BF16)
    act = act.reshape(tokens * top, hidden)
    ids_row = expert_ids[0].reshape(1, tokens * top)
    blocks = prep(ids_row, act, top, cap, local, grid.chips)
    acts = [blocks[0]]
    for k in range(1, grid.chips):
        acts.append(grid.move(blocks[k], lambda z, x, core, k=k: (z ^ (k // xs), x ^ (k % xs), core)))

    cots = spread(cotangent, quads)
    ups = (w_up[0], grid.move(w_up[0], across))
    downs = (w_down[0], grid.move(w_down[0], across))
    groups = 2 * local
    split = zs // 2 * xs
    halves = (range(split), range(split, grid.chips))
    parts, slot_rows = [None] * grid.chips, []
    for members in halves:
        some, held = token_grads(
            [acts[k] for k in members], [cots[k] for k in members], ups, downs, cap, local
        )
        slot_rows.append(held)
        for k, part in zip(members, some):
            parts[k] = part

    def total(*values):
        return functools.reduce(jnp.add, [v.astype(F32) for v in values]).astype(BF16)

    rows = [None] * zs
    if quads:
        rows[1] = parts[xs]
        for d in range(1, xs):
            parts[d] = total(parts[d], grid.move(parts[xs + d], along_z(1)))
    for z in reversed(range(zs)):
        if rows[z] is None:
            arrived = [grid.move(parts[z * xs + d], along_x(d)) for d in range(1, xs)]
            rows[z] = total(parts[z * xs], *arrived)
    if quads:
        rows[2] = total(rows[2], grid.move(rows[3], inward))
        last = [grid.move(rows[3], middle, -1), grid.move(rows[2], along_z(2), -1), grid.move(rows[1], along_z(1), -1)]
    else:
        last = [grid.move(rows[d], along_z(d), -1) for d in range(1, zs)]
    last.append(grid.move(rows[0], along_z(0), -1))
    delivered = total(*last)[None]

    x_rows = []
    for members in halves:
        x_rows.append(gather([acts[k] for k in members], [tokens_all[k] for k in members], cap, groups))

    def rows_of(h, p):
        grad, cot, act = slot_rows[h]
        return [(x_rows[h][p], 0), (act, p * local), (grad, p * local), (cot, p * local)]

    near_half = []
    for p in range(2):
        near_half.append(weight_grads([rows_of(0, p)], ups[p]))
    given = [grid.move(near_half[1][0], across), grid.move(near_half[1][1], across)]
    sent = [grid.move(v[j:j + local], across) for v, j in rows_of(1, 1)]
    ours = weight_grads([rows_of(1, 0), [(v, 0) for v in sent]], ups[0], [*near_half[0], *given])
    grad_up, grad_down = ours
    return (delivered, grad_up[None], grad_down[None])


def solution(mesh):
    return jax.shard_map(
        body,
        mesh=mesh,
        in_specs=(
            P("section", "ep", None),
            P("section", "ep", None),
            P("section", "ep", None, None),
            P("section", "ep", None),
            P("section", "ep", None),
            P("section", "ep", None, None),
            P("section", "ep", None, None),
        ),
        out_specs=(
            P("section", "ep", None),
            P("section", "ep", None, None),
            P("section", "ep", None, None),
        ),
        check_vma=False,
    )
```
